32 devices in a mesh: etp: 4 (over z), ep: 8 (over y, x, core).
Axes of the slice: x: 2, y: 2, z: 4, core: 2. Of those that a mesh axis runs over, the one named last changes fastest.
Arguments:
- x_norm: bfloat16 [8192, 1536], P('ep')
- expert_ids: int32 [8192, 6], P('ep')
- sel_scores: float32 [8192, 6], P('ep')
- w_gate: bfloat16 [64, 1536, 512], P('ep', None, 'etp')
- w_up: bfloat16 [64, 1536, 512], P('ep', None, 'etp')
- w_down: bfloat16 [64, 512, 1536], P('ep', 'etp')
- ws_gate: bfloat16 [1536, 1024], P(None, 'etp')
- ws_up: bfloat16 [1536, 1024], P(None, 'etp')
- ws_down: bfloat16 [1024, 1536], P('etp')
- d_out: bfloat16 [8192, 1536], P('ep')
Outputs:
- output 1: bfloat16 [8192, 1536], P('ep')
- output 2: float32 [8192, 1536], P('ep')
- output 3: float32 [8192, 6], P('ep')
- output 4: float32 [64, 1536, 512], P('ep', None, 'etp')
- output 5: float32 [64, 1536, 512], P('ep', None, 'etp')
- output 6: float32 [64, 512, 1536], P('ep', 'etp')
- output 7: float32 [1536, 1024], P(None, 'etp')
- output 8: float32 [1536, 1024], P(None, 'etp')
- output 9: float32 [1024, 1536], P('etp')
All inputs are finite; a program needn't handle non-finite values.
Results may differ from the reference program's by a relative error of at most 0.0120727.
Values are sent between devices in bfloat16 or wider.
A program may use at most 1 GiB of HBM per device.

```python
import jax
import jax.numpy as jnp
from jax import lax

HIDDEN = 1536
EXPERTS = 64
EXPERT_FF = 512
SHARED_FF = 1024
TOP_K = 6
TOK_DEV = 1024
EP_SIZE = 8
TOKENS = TOK_DEV * EP_SIZE
MEAN_LOAD = TOK_DEV * TOP_K // EXPERTS
CAPACITY = 2 * MEAN_LOAD - 1
ROUTE_SCALE = 2.5


def draw_expert_ids(key):
    perm_key, shard_key = jax.random.split(key)
    relabel = jax.random.permutation(perm_key, EXPERTS)

    def one_shard(sub_key):
        spread_key, row_key = jax.random.split(sub_key)
        spread = jax.random.randint(spread_key, (EXPERTS // 2,), 0, MEAN_LOAD)
        spread = spread.at[0].set(MEAN_LOAD - 1)
        counts = jnp.stack([MEAN_LOAD + spread, MEAN_LOAD - spread], axis=1).reshape(EXPERTS)
        run_ends = jnp.cumsum(counts)
        slot_index = jnp.arange(TOK_DEV * TOP_K)
        listed = jnp.sum(run_ends[None, :] <= slot_index[:, None], axis=1)
        chosen = relabel[listed].reshape(TOP_K, TOK_DEV).T
        row_order = jax.random.permutation(row_key, TOK_DEV)
        return chosen[row_order]

    shard_ids = jax.vmap(one_shard)(jax.random.split(shard_key, EP_SIZE))
    return shard_ids.reshape(TOKENS, TOP_K).astype(jnp.int32)


def setup_inputs(seed: int = 0) -> dict:
    keys = jax.random.split(jax.random.key(seed), 10)
    x_norm = jax.random.normal(keys[0], (TOKENS, HIDDEN), jnp.float32).astype(jnp.bfloat16)
    expert_ids = draw_expert_ids(keys[1])
    sel_scores = jax.nn.sigmoid(1.5 * jax.random.normal(keys[2], (TOKENS, TOP_K), jnp.float32))
    w_gate = (jax.random.normal(keys[3], (EXPERTS, HIDDEN, EXPERT_FF), jnp.float32) * HIDDEN ** -0.5).astype(jnp.bfloat16)
    w_up = (jax.random.normal(keys[4], (EXPERTS, HIDDEN, EXPERT_FF), jnp.float32) * HIDDEN ** -0.5).astype(jnp.bfloat16)
    w_down = (jax.random.normal(keys[5], (EXPERTS, EXPERT_FF, HIDDEN), jnp.float32) * EXPERT_FF ** -0.5).astype(jnp.bfloat16)
    ws_gate = (jax.random.normal(keys[6], (HIDDEN, SHARED_FF), jnp.float32) * HIDDEN ** -0.5).astype(jnp.bfloat16)
    ws_up = (jax.random.normal(keys[7], (HIDDEN, SHARED_FF), jnp.float32) * HIDDEN ** -0.5).astype(jnp.bfloat16)
    ws_down = (jax.random.normal(keys[8], (SHARED_FF, HIDDEN), jnp.float32) * SHARED_FF ** -0.5).astype(jnp.bfloat16)
    d_out = jax.random.normal(keys[9], (TOKENS, HIDDEN), jnp.float32).astype(jnp.bfloat16)
    return {'x_norm': x_norm, 'expert_ids': expert_ids, 'sel_scores': sel_scores, 'w_gate': w_gate, 'w_up': w_up, 'w_down': w_down, 'ws_gate': ws_gate, 'ws_up': ws_up, 'ws_down': ws_down, 'd_out': d_out}


def bf16_values(values):
    return values + lax.stop_gradient(values.astype(jnp.bfloat16).astype(jnp.float32) - values)


def reference(x_norm, expert_ids, sel_scores, w_gate, w_up, w_down, ws_gate, ws_up, ws_down, d_out):
    rows_max = EP_SIZE * CAPACITY
    flat_ids = expert_ids.reshape(-1)
    sort_order = jnp.argsort(flat_ids, stable=True)
    counts = jnp.bincount(flat_ids, length=EXPERTS)
    starts = jnp.cumsum(counts) - counts
    padded = jnp.concatenate([sort_order, jnp.zeros((rows_max,), sort_order.dtype)])
    row_index = jnp.arange(rows_max)

    def expert_rows(expert):
        picked = lax.dynamic_slice(padded, (starts[expert],), (rows_max,))
        return picked, row_index < counts[expert]

    picked_rows, live_rows = jax.vmap(expert_rows)(jnp.arange(EXPERTS))

    def forward(x_in, scores, wg_all, wu_all, wd_all, sg_mat, su_mat, sd_mat):
        gates = ROUTE_SCALE * scores / jnp.sum(scores, axis=-1, keepdims=True)
        gate_flat = gates.reshape(-1)

        def expert_step(routed_acc, inputs):
            picked, live_mask, wg_one, wu_one, wd_one = inputs
            tok_rows = picked // TOP_K
            x_rows = x_in[tok_rows]
            gate_act = jnp.dot(x_rows, wg_one, preferred_element_type=jnp.float32)
            up_lin = jnp.dot(x_rows, wu_one, preferred_element_type=jnp.float32)
            hidden = bf16_values(jax.nn.silu(gate_act) * up_lin)
            out_rows = jnp.dot(hidden, wd_one, preferred_element_type=jnp.float32)
            weight = jnp.where(live_mask, gate_flat[picked], 0.0)
            return routed_acc.at[tok_rows].add(out_rows * weight[:, None]), None

        routed, _ = lax.scan(jax.checkpoint(expert_step), jnp.zeros((TOKENS, HIDDEN), jnp.float32), (picked_rows, live_rows, wg_all, wu_all, wd_all))
        shared_act = jnp.dot(x_in, sg_mat, preferred_element_type=jnp.float32)
        shared_lin = jnp.dot(x_in, su_mat, preferred_element_type=jnp.float32)
        shared_hid = bf16_values(jax.nn.silu(shared_act) * shared_lin)
        return routed + jnp.dot(shared_hid, sd_mat, preferred_element_type=jnp.float32)

    y_full, pullback = jax.vjp(forward, x_norm.astype(jnp.float32), sel_scores, w_gate.astype(jnp.float32), w_up.astype(jnp.float32), w_down.astype(jnp.float32), ws_gate.astype(jnp.float32), ws_up.astype(jnp.float32), ws_down.astype(jnp.float32))
    grads = pullback(d_out.astype(jnp.float32))
    return (y_full.astype(jnp.bfloat16), grads[0], grads[1], grads[2], grads[3], grads[4], grads[5], grads[6], grads[7])
```

```python
import functools

import jax
import jax.numpy as jnp
from jax import lax
from jax.experimental import pallas as pl
from jax.experimental.pallas import tpu as pltpu
from jax.sharding import PartitionSpec as P

ROUTE_SCALE = 2.5


def gate_weights(scores):
    return ROUTE_SCALE * scores / jnp.sum(scores, axis=-1, keepdims=True)


def expert_kernel(num_pairs, row_tile, num_y, num_dx, use_gate, *refs):
    x_ref, dy_ref, g_ref, wgu_ref, wgut_ref, wd_ref, wdt_ref = refs[:7]
    y_adds = refs[7:7 + num_y]
    dx_adds = refs[7 + num_y:7 + num_y + num_dx]
    y_ref, dx_ref, dab_ref, gh_ref, dg_ref, y_acc, dx_acc = refs[7 + num_y + num_dx:]
    pair = pl.program_id(0)
    rows = x_ref.shape[0]

    def tile_step(tile, carry):
        span = pl.ds(pl.multiple_of(tile * row_tile, row_tile), row_tile)
        x = x_ref[span, :]
        dy = dy_ref[span, :]
        d_raw = jnp.dot(dy, wdt_ref[0], preferred_element_type=jnp.float32)
        lane = lax.broadcasted_iota(jnp.int32, (row_tile, 8), 1)
        dg = jnp.zeros((row_tile, 8), jnp.float32)
        gh_parts, dab_parts = [], []
        for j in range(2):
            ab = jnp.dot(x, wgu_ref[j], preferred_element_type=jnp.float32)
            a, b = ab[:, :128], ab[:, 128:]
            d_e = d_raw[:, j * 128:(j + 1) * 128]
            logistic = jax.nn.sigmoid(a)
            silu_val = a * logistic
            silu_grad = logistic * (1.0 + a * (1.0 - logistic))
            hidden = (silu_val * b).astype(jnp.bfloat16)
            hidden_f = hidden.astype(jnp.float32)
            if use_gate:
                gate = jnp.sum(jnp.where(lane == 2 * pair + j, g_ref[0, span, :], 0.0), axis=1, keepdims=True)
                gate = jnp.broadcast_to(gate, a.shape)
                live = gate != 0.0
                gh = jnp.where(live, gate * hidden_f, 0.0).astype(jnp.bfloat16)
                dh = gate * d_e
                da = jnp.where(live, dh * b * silu_grad, 0.0)
                db = jnp.where(live, dh * silu_val, 0.0)
                score = jnp.sum(hidden_f * d_e, axis=1, keepdims=True)
                dg = dg + jnp.where(lane == 2 * pair + j, score, 0.0)
            else:
                gh = hidden
                da = d_e * b * silu_grad
                db = d_e * silu_val
            dab = jnp.concatenate([da.astype(jnp.bfloat16), db.astype(jnp.bfloat16)], axis=1)
            dab_ref[j, span, :] = dab
            gh_ref[j, span, :] = gh
            gh_parts.append(gh)
            dab_parts.append(dab)
        y_new = jnp.dot(jnp.concatenate(gh_parts, axis=1), wd_ref[0], preferred_element_type=jnp.float32)
        dx_new = jnp.dot(jnp.concatenate(dab_parts, axis=1), wgut_ref[0], preferred_element_type=jnp.float32)

        @pl.when(pair == 0)
        def _():
            y_sum, dx_sum = y_new, dx_new
            for add in y_adds:
                y_sum = y_sum + add[span, :].astype(jnp.float32)
            for add in dx_adds:
                dx_sum = dx_sum + add[span, :].astype(jnp.float32)
            y_acc[span, :] = y_sum
            dx_acc[span, :] = dx_sum
            dg_ref[span, :] = dg

        @pl.when(pair > 0)
        def _():
            y_acc[span, :] += y_new
            dx_acc[span, :] += dx_new
            dg_ref[span, :] += dg

        return carry

    lax.fori_loop(0, rows // row_tile, tile_step, 0)

    @pl.when(pair == num_pairs - 1)
    def _():
        y_ref[...] = y_acc[...].astype(y_ref.dtype)
        dx_ref[...] = dx_acc[...].astype(dx_ref.dtype)


def expert_pass(x, dy, gates, flip, weights, y_adds=(), dx_adds=(), out_dtype=jnp.bfloat16, name='experts'):
    wgu, wgut, wd, wdt = weights
    rows, hidden = x.shape
    num_pairs = wd.shape[0]
    row_tile = min(256, rows)
    use_gate = gates is not None
    if gates is None:
        gates = jnp.zeros((1, rows, 8), jnp.float32)
    once = pl.Buffered(1)
    whole = pl.BlockSpec((rows, hidden), lambda p: (0, 0), pipeline_mode=once)
    in_specs = [whole, whole, pl.BlockSpec((1, rows, 8), lambda p: (flip, 0, 0), pipeline_mode=once),
                pl.BlockSpec((2, hidden, 256), lambda p: (p, 0, 0)),
                pl.BlockSpec((1, 512, hidden), lambda p: (p, 0, 0)),
                pl.BlockSpec((1, 256, hidden), lambda p: (p, 0, 0)),
                pl.BlockSpec((1, hidden, 256), lambda p: (p, 0, 0))]
    in_specs += [whole] * (len(y_adds) + len(dx_adds))
    out_specs = [whole, whole,
                 pl.BlockSpec((2, rows, 256), lambda p: (p, 0, 0)),
                 pl.BlockSpec((2, rows, 128), lambda p: (p, 0, 0)),
                 pl.BlockSpec((rows, 8), lambda p: (0, 0))]
    out_shape = [jax.ShapeDtypeStruct((rows, hidden), out_dtype), jax.ShapeDtypeStruct((rows, hidden), out_dtype),
                 jax.ShapeDtypeStruct((2 * num_pairs, rows, 256), jnp.bfloat16),
                 jax.ShapeDtypeStruct((2 * num_pairs, rows, 128), jnp.bfloat16),
                 jax.ShapeDtypeStruct((rows, 8), jnp.float32)]
    flops = 14 * rows * hidden * 256 * num_pairs
    return pl.pallas_call(
        functools.partial(expert_kernel, num_pairs, row_tile, len(y_adds), len(dx_adds), use_gate),
        grid=(num_pairs,), in_specs=in_specs, out_specs=out_specs, out_shape=out_shape,
        scratch_shapes=[pltpu.VMEM((rows, hidden), jnp.float32), pltpu.VMEM((rows, hidden), jnp.float32)],
        compiler_params=pltpu.CompilerParams(dimension_semantics=('arbitrary',), vmem_limit_bytes=60 * 1024 * 1024),
        cost_estimate=pl.CostEstimate(flops=flops, bytes_accessed=20 * rows * hidden, transcendentals=rows * 256 * num_pairs),
        name=name,
    )(x, dy, gates, wgu, wgut, wd, wdt, *y_adds, *dx_adds)


def pack_weights(wg, wu, wd):
    num_exp, hidden, _ = wg.shape
    wgu = jnp.concatenate([wg, wu], axis=2)
    wgut = wgu.transpose(0, 2, 1).reshape(num_exp // 2, 512, hidden)
    wd_pair = wd.reshape(num_exp // 2, 256, hidden)
    return wgu, wgut, wd_pair, wd_pair.transpose(0, 2, 1)


def solution(mesh):
    ep_size = mesh.shape['ep']
    etp_size = mesh.shape['etp']
    row_spec = P('ep', None)
    col_spec = P('ep', None, 'etp')
    down_spec = P('ep', 'etp', None)
    in_specs = (row_spec, row_spec, row_spec, col_spec, col_spec, down_spec, P(None, 'etp'), P(None, 'etp'), P('etp', None), row_spec)
    out_specs = (row_spec, row_spec, row_spec, col_spec, col_spec, down_spec, P(None, 'etp'), P(None, 'etp'), P('etp', None))

    def send(value, flip):
        return lax.ppermute(value, 'ep', [(i, i ^ flip) for i in range(ep_size)])

    def device_step(x_local, ids_local, scores_local, wg_local, wu_local, wd_local, sg_local, su_local, sd_local, dy_local):
        rows, top_k = ids_local.shape
        hidden = x_local.shape[1]
        local_experts = wg_local.shape[0]
        num_experts = local_experts * ep_size
        me = lax.axis_index('ep')
        flips = me ^ jnp.arange(ep_size)

        x, dy = {0: x_local}, {0: dy_local}
        for f in (2, 4, 1):
            x[f], dy[f] = send(x_local, f), send(dy_local, f)
        x[6], dy[6] = send(x[2], 4), send(dy[4], 2)
        for f in (3, 5, 7):
            x[f], dy[f] = send(x[f ^ 1], 1), send(dy[f ^ 1], 1)

        gates = gate_weights(scores_local)
        chosen = ids_local.T[:, None, :] == jnp.arange(num_experts)[None, :, None]
        gate_rows = jnp.sum(jnp.where(chosen, gates.T[:, None, :], 0.0), axis=0)
        gate_recv = lax.all_to_all(gate_rows, 'ep', 0, 0, tiled=True).reshape(ep_size, local_experts, rows)
        gate_recv = gate_recv[flips].transpose(0, 2, 1)

        split = lambda mat: mat.reshape(hidden, 2, 128).transpose(1, 0, 2)
        shared_w = pack_weights(split(sg_local), split(su_local), sd_local.reshape(2, 128, hidden))
        routed_w = pack_weights(wg_local, wu_local, wd_local)

        y_sh, dx_sh, dab_sh, gh_sh, _ = expert_pass(x_local, dy_local, None, 0, shared_w, name='shared')
        dws_gu = jnp.einsum('td,etc->edc', x_local, dab_sh, preferred_element_type=jnp.float32)
        dws_d = jnp.einsum('etc,td->ecd', gh_sh, dy_local, preferred_element_type=jnp.float32)
        dws_gate = dws_gu[:, :, :128].transpose(1, 0, 2).reshape(hidden, 256)
        dws_up = dws_gu[:, :, 128:].transpose(1, 0, 2).reshape(hidden, 256)
        dws_gate, dws_up, dws_down = lax.psum((dws_gate, dws_up, dws_d.reshape(256, hidden)), 'ep')

        dab, gh, dg, y_back, dx_back = {}, {}, {}, {}, {}
        for f in (1, 3, 5, 7):
            y_f, dx_f, dab[f], gh[f], dg[f] = expert_pass(x[f], dy[f], gate_recv, f, routed_w)
            y_mate, dx_mate = send(y_f, 1), send(dx_f, 1)
            f -= 1
            y_adds = (y_mate, y_sh) if f == 0 else (y_mate,)
            dx_adds = (dx_mate, dx_sh) if f == 0 else (dx_mate,)
            y_f, dx_f, dab[f], gh[f], dg[f] = expert_pass(x[f], dy[f], gate_recv, f, routed_w, y_adds, dx_adds)
            y_back[f] = send(y_f, f) if f else y_f
            dx_back[f] = send(dx_f, f) if f else dx_f

        def etp_sum(parts):
            total = sum(parts[f].astype(jnp.float32) for f in (0, 2, 4, 6)).astype(jnp.bfloat16)
            pieces = lax.all_to_all(total, 'etp', 0, 0, tiled=True).reshape(etp_size, rows // etp_size, hidden)
            return jnp.sum(pieces.astype(jnp.float32), axis=0)

        y_out = lax.all_gather(etp_sum(y_back).astype(jnp.bfloat16), 'etp', axis=0, tiled=True)
        dx_norm = lax.all_gather(etp_sum(dx_back), 'etp', axis=0, tiled=True)

        dg_send = jnp.stack([dg[f].T for f in range(ep_size)])[flips].reshape(num_experts, rows)
        dg_all = lax.all_to_all(dg_send, 'ep', 0, 0, tiled=True)
        gate_grad = jnp.sum(jnp.where(chosen, dg_all[None], 0.0), axis=1).T
        gate_grad = lax.psum(gate_grad, 'etp')
        _, gate_pull = jax.vjp(gate_weights, scores_local)
        d_scores = gate_pull(gate_grad)[0]

        order = range(ep_size)
        x_all = jnp.concatenate([x[f] for f in order], axis=0)
        dy_all = jnp.concatenate([dy[f] for f in order], axis=0)
        dab_all = jnp.concatenate([dab[f] for f in order], axis=1)
        gh_all = jnp.concatenate([gh[f] for f in order], axis=1)
        dw_gu = jnp.einsum('td,etc->edc', x_all, dab_all, preferred_element_type=jnp.float32)
        dw_down = jnp.einsum('etc,td->ecd', gh_all, dy_all, preferred_element_type=jnp.float32)
        return (y_out, dx_norm, d_scores, dw_gu[:, :, :128], dw_gu[:, :, 128:], dw_down, dws_gate, dws_up, dws_down)

    return jax.shard_map(device_step, mesh=mesh, in_specs=in_specs, out_specs=out_specs, check_vma=False)
```

```python
import functools

import jax
import jax.numpy as jnp
from jax import lax
from jax.experimental import pallas as pl
from jax.experimental.pallas import tpu as pltpu
from jax.sharding import PartitionSpec as P

ROUTE_SCALE = 2.5
ROW_TILE = 256


def gate_weights(scores):
    return ROUTE_SCALE * scores / jnp.sum(scores, axis=-1, keepdims=True)


def forward_kernel(num_exp, num_adds, gated, packed, num_deps, *refs):
    x_ref, g_ref, wgu_ref, wd_ref = refs[:4]
    adds = refs[4:4 + num_adds]
    outs = refs[4 + num_adds + num_deps:]
    y_ref, ab_ref, gh_ref = outs[:3]
    x = x_ref[...]
    gh_parts = []
    for e in range(num_exp):
        ab = jnp.dot(x, wgu_ref[e], preferred_element_type=jnp.float32)
        ab_ref[:, e * 256:(e + 1) * 256] = ab
        a, b = ab[:, :128], ab[:, 128:]
        hidden = (a * jax.nn.sigmoid(a) * b).astype(jnp.bfloat16)
        if gated:
            gate = jnp.broadcast_to(g_ref[0, :, e:e + 1], a.shape)
            hidden = jnp.where(gate != 0.0, gate * hidden.astype(jnp.float32), 0.0).astype(jnp.bfloat16)
        gh_ref[:, e * 128:(e + 1) * 128] = hidden
        gh_parts.append(hidden)
    y = jnp.dot(jnp.concatenate(gh_parts, axis=1), wd_ref[...], preferred_element_type=jnp.float32)
    for add in adds:
        y = y + add[...].astype(jnp.float32)
    y_ref[...] = y.astype(y_ref.dtype)
    if packed:
        outs[3][...] = x


def backward_kernel(num_exp, num_adds, gated, packed, num_deps, *refs):
    dy_ref, g_ref, ab_ref, wdt_ref, wgut_ref = refs[:5]
    adds = refs[5:5 + num_adds]
    outs = refs[5 + num_adds + num_deps:]
    dx_ref, dg_ref, dab_ref = outs[:3]
    dy = dy_ref[...]
    lane = lax.broadcasted_iota(jnp.int32, dg_ref.shape, 1)
    dg = jnp.zeros(dg_ref.shape, jnp.float32)
    dab_parts = []
    for e in range(num_exp):
        if e % 2 == 0:
            d_pair = jnp.dot(dy, wdt_ref[:, e * 128:(e + 2) * 128], preferred_element_type=jnp.float32)
        d_e = d_pair[:, (e % 2) * 128:(e % 2 + 1) * 128]
        a, b = ab_ref[:, e * 256:e * 256 + 128], ab_ref[:, e * 256 + 128:(e + 1) * 256]
        logistic = jax.nn.sigmoid(a)
        silu_val = a * logistic
        silu_grad = logistic * (1.0 + a * (1.0 - logistic))
        if gated:
            hidden = (silu_val * b).astype(jnp.bfloat16).astype(jnp.float32)
            score = jnp.sum(hidden * d_e, axis=1, keepdims=True)
            dg = dg + jnp.where(lane == e, score, 0.0)
            gate = jnp.broadcast_to(g_ref[0, :, e:e + 1], a.shape)
            live = gate != 0.0
            dh = gate * d_e
            da = jnp.where(live, dh * b * silu_grad, 0.0)
            db = jnp.where(live, dh * silu_val, 0.0)
        else:
            da = d_e * b * silu_grad
            db = d_e * silu_val
        dab = jnp.concatenate([da.astype(jnp.bfloat16), db.astype(jnp.bfloat16)], axis=1)
        dab_ref[:, e * 256:(e + 1) * 256] = dab
        dab_parts.append(dab)
    dx = jnp.dot(jnp.concatenate(dab_parts, axis=1), wgut_ref[...], preferred_element_type=jnp.float32)
    for add in adds:
        dx = dx + add[...].astype(jnp.float32)
    dx_ref[...] = dx.astype(dx_ref.dtype)
    dg_ref[...] = dg
    if packed:
        outs[3][...] = dy


def whole_spec(arr):
    return pl.BlockSpec(arr.shape, lambda t: (0,) * len(arr.shape), pipeline_mode=pl.Buffered(1))


def row_tiles(rows, cols, base=0):
    tile = min(ROW_TILE, rows)
    return pl.BlockSpec((tile, cols), lambda t: (base * (rows // tile) + t, 0))


def gate_spec(rows, flip):
    return pl.BlockSpec((1, min(ROW_TILE, rows), 8), lambda t: (flip, t, 0))


def run_kernel(body, rows, arrays, specs, bufs, deps, outs, buf_outs, flops):
    any_spec = pl.BlockSpec(memory_space=pl.ANY)
    extra = list(bufs) + list(deps)
    aliases = {}
    for k, buf in enumerate(bufs):
        aliases[len(arrays) + k] = len(outs) - len(buf_outs) + k
    all_outs = outs
    return pl.pallas_call(
        functools.partial(body, len(extra)),
        grid=(rows // min(ROW_TILE, rows),),
        in_specs=list(specs) + [any_spec] * len(extra),
        out_specs=[spec for _, _, spec in all_outs],
        out_shape=[jax.ShapeDtypeStruct(shape, dtype) for shape, dtype, _ in all_outs],
        input_output_aliases=aliases,
        compiler_params=pltpu.CompilerParams(dimension_semantics=('arbitrary',), vmem_limit_bytes=56 * 1024 * 1024),
        cost_estimate=pl.CostEstimate(flops=flops, bytes_accessed=flops // 1000, transcendentals=0),
    )(*arrays, *extra)


def forward_pass(x, gates, flip, weights, adds=(), bufs=None, deps=(), out_dtype=jnp.bfloat16, shards=0):
    wgu, wd = weights
    rows, hidden = x.shape
    num_exp = wgu.shape[0]
    gated = gates is not None
    if not gated:
        gates, flip = jnp.zeros((1, rows, 8), jnp.float32), 0
    tile = row_tiles(rows, hidden)
    arrays = [x, gates, wgu, wd, *adds]
    specs = [tile, gate_spec(rows, flip), whole_spec(wgu), whole_spec(wd)] + [tile] * len(adds)
    slot = flip if shards else 0
    outs = [((rows, hidden), out_dtype, tile), ((rows, num_exp * 256), jnp.float32, row_tiles(rows, num_exp * 256)),
            ((max(shards, 1) * rows, num_exp * 128), jnp.bfloat16, row_tiles(rows, num_exp * 128, slot))]
    buf_outs = []
    if shards:
        outs.append(((shards * rows, hidden), jnp.bfloat16, row_tiles(rows, hidden, slot)))
        buf_outs = outs[2:]
    body = lambda num_deps, *refs: forward_kernel(num_exp, len(adds), gated, bool(shards), num_deps, *refs)
    return run_kernel(body, rows, arrays, specs, bufs or (), deps, outs, buf_outs, 6 * rows * hidden * 128 * num_exp)


def backward_pass(dy, gates, flip, ab, weights, adds=(), bufs=None, deps=(), out_dtype=jnp.bfloat16, shards=0):
    wdt, wgut = weights
    rows, hidden = dy.shape
    num_exp = wdt.shape[1] // 128
    gated = gates is not None
    if not gated:
        gates, flip = jnp.zeros((1, rows, 8), jnp.float32), 0
    tile = row_tiles(rows, hidden)
    arrays = [dy, gates, ab, wdt, wgut, *adds]
    specs = [tile, gate_spec(rows, flip), row_tiles(rows, num_exp * 256), whole_spec(wdt), whole_spec(wgut)] + [tile] * len(adds)
    slot = flip if shards else 0
    outs = [((rows, hidden), out_dtype, tile), ((rows, 8), jnp.float32, row_tiles(rows, 8)),
            ((max(shards, 1) * rows, num_exp * 256), jnp.bfloat16, row_tiles(rows, num_exp * 256, slot))]
    buf_outs = []
    if shards:
        outs.append(((shards * rows, hidden), jnp.bfloat16, row_tiles(rows, hidden, slot)))
        buf_outs = outs[2:]
    body = lambda num_deps, *refs: backward_kernel(num_exp, len(adds), gated, bool(shards), num_deps, *refs)
    return run_kernel(body, rows, arrays, specs, bufs or (), deps, outs, buf_outs, 8 * rows * hidden * 128 * num_exp)


def pack_weights(wg, wu, wd):
    num_exp, hidden, _ = wg.shape
    wgu = jnp.concatenate([wg, wu], axis=2)
    wgut = wgu.transpose(0, 2, 1).reshape(num_exp * 256, hidden)
    wd2 = wd.reshape(num_exp * 128, hidden)
    return (wgu, wd2), (wd2.T, wgut)


def solution(mesh):
    ep_size = mesh.shape['ep']
    etp_size = mesh.shape['etp']
    row_spec = P('ep', None)
    col_spec = P('ep', None, 'etp')
    down_spec = P('ep', 'etp', None)
    in_specs = (row_spec, row_spec, row_spec, col_spec, col_spec, down_spec, P(None, 'etp'), P(None, 'etp'), P('etp', None), row_spec)
    out_specs = (row_spec, row_spec, row_spec, col_spec, col_spec, down_spec, P(None, 'etp'), P(None, 'etp'), P('etp', None))

    def send(value, flip):
        return lax.ppermute(value, 'ep', [(i, i ^ flip) for i in range(ep_size)])

    def block_step(x_local, ids_local, scores_local, wg_local, wu_local, wd_local, sg_local, su_local, sd_local, dy_local):
        rows, _ = ids_local.shape
        hidden = x_local.shape[1]
        local_experts = wg_local.shape[0]
        num_experts = local_experts * ep_size
        me = lax.axis_index('ep')
        flips = me ^ jnp.arange(ep_size)
        quarter = rows // etp_size

        gates = gate_weights(scores_local)
        chosen = ids_local.T[:, None, :] == jnp.arange(num_experts)[None, :, None]
        gate_rows = jnp.sum(jnp.where(chosen, gates.T[:, None, :], 0.0), axis=0)
        gate_recv = lax.all_to_all(gate_rows, 'ep', 0, 0, tiled=True)
        gate_recv = gate_recv.reshape(ep_size, local_experts, rows)[flips].transpose(0, 2, 1)

        def share(local):
            mine = lax.dynamic_slice_in_dim(local, lax.axis_index('etp') * quarter, quarter, axis=0)
            got = {0: local}
            corner = send(mine, 6)
            for f in (1, 2, 4):
                got[f] = send(local, f)
            got[6] = lax.all_gather(corner, 'etp', axis=0, tiled=True)
            for f in (3, 5, 7):
                got[f] = send(got[f ^ 1], 1)
            return got

        x, dy = share(x_local), share(dy_local)

        split = lambda mat: mat.reshape(hidden, 2, 128).transpose(1, 0, 2)
        shared_fwd, shared_bwd = pack_weights(split(sg_local), split(su_local), sd_local.reshape(2, 128, hidden))
        routed_fwd, routed_bwd = pack_weights(wg_local, wu_local, wd_local)

        y_sh, ab_sh, gh_sh = forward_pass(x_local, None, 0, shared_fwd)
        dx_sh, _, dab_sh = backward_pass(dy_local, None, 0, ab_sh, shared_bwd)

        ab, dg, y_back, dx_back = {}, {}, {}, {}
        bufs, deps = None, (dx_sh,)
        for f in (1, 3, 5, 7):
            y_f, ab[f], *bufs = forward_pass(x[f], gate_recv, f, routed_fwd, (), bufs, deps, shards=ep_size)
            deps = ()
            adds = (send(y_f, 1),) + ((y_sh,) if f == 1 else ())
            f -= 1
            y_f, ab[f], *bufs = forward_pass(x[f], gate_recv, f, routed_fwd, adds, bufs, shards=ep_size)
            y_back[f] = send(y_f, f) if f else y_f
        gh_all, x_all = bufs

        def etp_exchange(parts):
            total = sum(parts[f].astype(jnp.float32) for f in (0, 2, 4, 6)).astype(jnp.bfloat16)
            pieces = lax.all_to_all(total, 'etp', 0, 0, tiled=True)
            return jnp.sum(pieces.reshape(etp_size, quarter, hidden).astype(jnp.float32), axis=0)

        y_piece = etp_exchange(y_back).astype(jnp.bfloat16)
        y_out = lax.all_gather(y_piece, 'etp', axis=0, tiled=True)

        bufs, deps = None, (gh_all,)
        for f in (7, 5, 3, 1):
            dx_f, dg[f], *bufs = backward_pass(dy[f], gate_recv, f, ab[f], routed_bwd, (), bufs, deps, shards=ep_size)
            deps = ()
            adds = (send(dx_f, 1),) + ((dx_sh,) if f == 1 else ())
            f -= 1
            dx_f, dg[f], *bufs = backward_pass(dy[f], gate_recv, f, ab[f], routed_bwd, adds, bufs,
                                               (y_piece,) if f == 0 else (), shards=ep_size)
            dx_back[f] = send(dx_f, f) if f else dx_f
        dab_all, dy_all = bufs

        dx_norm = lax.all_gather(etp_exchange(dx_back), 'etp', axis=0, tiled=True)

        dg_send = jnp.stack([dg[f].T for f in range(ep_size)])[flips].reshape(num_experts, rows)
        dg_all = lax.all_to_all(dg_send, 'ep', 0, 0, tiled=True)
        gate_grad = jnp.sum(jnp.where(chosen, dg_all[None], 0.0), axis=1)
        gate_grad = lax.psum(gate_grad, 'etp').T
        _, gate_pull = jax.vjp(gate_weights, scores_local)
        d_scores = gate_pull(gate_grad)[0]

        def up_grads(xs, dabs):
            grad = jnp.einsum('td,tc->dc', xs, dabs, preferred_element_type=jnp.float32)
            return grad.reshape(hidden, dabs.shape[1] // 256, 2, 128)

        def down_grad(ghs, dys):
            return jnp.einsum('tc,td->cd', ghs, dys, preferred_element_type=jnp.float32)

        dws_gu = up_grads(x_local, dab_sh).transpose(2, 0, 1, 3).reshape(2, hidden, 256)
        dws_down = down_grad(gh_sh, dy_local)
        dws_gate, dws_up, dws_down = lax.psum((dws_gu[0], dws_gu[1], dws_down), 'ep')

        dw_gu = up_grads(x_all, dab_all)
        dw_down = down_grad(gh_all, dy_all).reshape(local_experts, 128, hidden)
        dw_gate, dw_up = dw_gu[:, :, 0].transpose(1, 0, 2), dw_gu[:, :, 1].transpose(1, 0, 2)
        return (y_out, dx_norm, d_scores, dw_gate, dw_up, dw_down, dws_gate, dws_up, dws_down)

    return jax.shard_map(block_step, mesh=mesh, in_specs=in_specs, out_specs=out_specs, check_vma=False)
```
